128 devices in a mesh: blk: 16 (over z, x_hi, core), head: 8 (over y, x_lo).
Axes of the slice: x: 4 (x_hi: 2, x_lo: 2; x = x_hi * 2 + x_lo), y: 4, z: 4, core: 2. Of those that a mesh axis runs over, the one named last changes fastest.
Arguments:
- queries: bfloat16 [4096, 8192], P('blk', 'head'), may hold values from -4 to 10
- context_keys: bfloat16 [16384, 1024], P('blk', 'head'), may hold values from -4 to 7
- context_values: bfloat16 [16384, 1024], P('blk', 'head'), may hold values from -6 to 6
- response_keys: bfloat16 [4096, 1024], P('blk', 'head'), may hold values from -4 to 7
- response_values: bfloat16 [4096, 1024], P('blk', 'head'), may hold values from -6 to 6
- out_weight: bfloat16 [8192, 8192], P('head', 'blk'), may hold values from -0.09375 to 0.09375
- query_docs: int32 [32], replicated, may hold values from 0 to 2
- block_docs: int32 [128], replicated, may hold values from 0 to 2
- visits: int32 [32, 4, 8], replicated, may hold values 0 or 1
Outputs:
- mixed: bfloat16 [4096, 8192], P('blk', 'head')
The draws below stay inside these ranges and needn't reach their ends.
All inputs are finite; a program needn't handle non-finite values.
Results may differ from the reference program's by a relative error of at most 0.0165.
Values may be sent and summed in bfloat16 or wider, within the bound.
No kernel may reach another device: no remote copies, remote signals or barrier semaphores. Data moves between devices by JAX's collectives and lax.ppermute only.
A program may use at most 128 MiB of HBM per device.

```python
import jax
import jax.numpy as jnp
from jax import lax

D = 8192
HQ = 64
KVH = 8
HD = 128
BLOCK = 128
HOPS = 3
DOCS = 3
TOK_DEV = 256
CTX_DEV = 1024
TOKENS = 4096
CTX = 16384
QBLOCKS = 32
CBLOCKS = 128
KVB = 8
N_BLK = 16


def draw_queries(key, part):
    values = jnp.clip(jax.random.normal(key, (TOKENS, HQ * HD), jnp.float32), -4.0, 4.0)
    return values.astype(jnp.bfloat16)


def draw_context_keys(key, part):
    values = jnp.clip(jax.random.normal(key, (CTX, KVH * HD), jnp.float32), -4.0, 4.0)
    return values.astype(jnp.bfloat16)


def draw_response_keys(key, part):
    values = jnp.clip(jax.random.normal(jax.random.fold_in(key, 11), (TOKENS, KVH * HD), jnp.float32), -4.0, 4.0)
    return values.astype(jnp.bfloat16)


def plant(entries, stream_key, least, largest):
    longest = entries.shape.index(max(entries.shape))
    spots = []
    for shift in (0, 1):
        where = [jax.random.randint(jax.random.fold_in(stream_key, axis), (), 0, length) for axis, length in enumerate(entries.shape)]
        where[longest] = (where[longest] + shift) % entries.shape[longest]
        spots.append(tuple(where))
    return entries.at[spots[0]].set(least).at[spots[1]].set(largest)


def spiked(values, own_key, source, target, blocks, factor):
    owner, partner = [(jnp.arange(values.shape[position]) // (values.shape[position] // blocks)).reshape([-1 if axis == position else 1 for axis in range(values.ndim)]) for position in (source, target)]
    chosen = jax.random.permutation(own_key, blocks)[partner]
    strong = (owner == chosen) | (owner == (partner + blocks // 2) % blocks)
    return jnp.where(strong, factor * values, values)


def shard_levels(key, shape, pieces, smallest, largest):
    level = 1.0
    for position, shards_of in pieces:
        heights = jax.random.uniform(jax.random.fold_in(jax.random.fold_in(key, 6), position), (shards_of,), jnp.float32, smallest / len(pieces), largest / len(pieces))
        level = level * jnp.repeat(jnp.exp(heights), shape[position] // shards_of).reshape((-1,) + (1,) * (len(shape) - 1 - position))
    return level


def centred(key, dims, deviation, bound, split=(), kind=jnp.bfloat16):
    array = jax.random.normal(key, dims, jnp.float32) * deviation
    if len(split) > 0:
        array = shard_levels(key, dims, split, -0.22, 0.18) * array
    return jnp.clip(array, min=-bound, max=bound).astype(kind)


def bell_draw_with(rng, extent, deviation, bound, cuts, heavy, kind=jnp.bfloat16):
    entries = deviation * jax.random.normal(rng, extent, jnp.float32)
    if cuts:
        entries = entries * shard_levels(rng, extent, cuts, -0.22, 0.18)
    return jnp.clip(spiked(entries, jax.random.fold_in(rng, 3), *heavy), -bound, bound).astype(kind)


def setup_inputs(seed: int = 0) -> dict:
    streams_of = jax.random.split(jax.random.key(seed), 10)
    return {
        "queries": draw_queries(jax.random.fold_in(streams_of[9], 71), 0),
        "context_keys": draw_context_keys(jax.random.fold_in(streams_of[9], 71), 0),
        "context_values": centred(streams_of[2], (CTX, KVH * HD), 1.0, 6.0, ((0, 16), (1, 8))),
        "response_keys": draw_response_keys(jax.random.fold_in(streams_of[9], 71), 0),
        "response_values": centred(streams_of[4], (TOKENS, KVH * HD), 1.0, 6.0, ((0, 16), (1, 8))),
        "out_weight": bell_draw_with(streams_of[5], (HQ * HD, D), (HQ * HD) ** -0.5, 0.09375, ((0, 8), (1, 16)), (0, 1, 16, 2.0)),
        "query_docs": plant(jax.random.randint(streams_of[6], (QBLOCKS,), 0, DOCS), jax.random.fold_in(streams_of[6], 1), 0, DOCS - 1).astype(jnp.int32),
        "block_docs": plant(jax.random.randint(streams_of[7], (CBLOCKS,), 0, DOCS), jax.random.fold_in(streams_of[7], 1), 0, DOCS - 1).astype(jnp.int32),
        "visits": plant((jax.random.randint(streams_of[8], (QBLOCKS, HOPS + 1, KVB), 0, 2) < 1).astype(jnp.int32), jax.random.fold_in(streams_of[8], 1), 0, 1),
    }


def reference(queries, context_keys, context_values, response_keys, response_values, out_weight, query_docs, block_docs, visits):
    per_group = HQ // KVH
    softmax_scale = HD ** -0.5
    query_heads = queries.reshape(N_BLK, TOK_DEV, KVH, per_group, HD)
    key_shards = context_keys.reshape(N_BLK, CTX_DEV, KVH, HD)
    value_shards = context_values.reshape(N_BLK, CTX_DEV, KVH, HD)
    own_keys = response_keys.reshape(N_BLK, TOK_DEV, KVH, HD)
    own_values = response_values.reshape(N_BLK, TOK_DEV, KVH, HD)
    query_doc = query_docs.reshape(N_BLK, TOK_DEV // BLOCK)
    block_doc = block_docs.reshape(N_BLK, KVB)
    visited = visits.reshape(N_BLK, TOK_DEV // BLOCK, HOPS + 1, KVB)
    row_block = (jnp.arange(TOK_DEV) // BLOCK).astype(jnp.int32)
    key_block = (jnp.arange(CTX_DEV) // BLOCK).astype(jnp.int32)
    positions = jnp.arange(TOK_DEV)
    causal = positions[:, None] >= positions[None, :]

    def one_shard(anchor):
        holders = ((anchor + jnp.arange(HOPS + 1)) % N_BLK).astype(jnp.int32)
        all_keys = jnp.concatenate([key_shards[holders].reshape((HOPS + 1) * CTX_DEV, KVH, HD), own_keys[anchor]], axis=0)
        all_values = jnp.concatenate([value_shards[holders].reshape((HOPS + 1) * CTX_DEV, KVH, HD), own_values[anchor]], axis=0)
        visit_rows = visited[anchor][row_block] == 1
        doc_match = block_doc[holders][None, :, :] == query_doc[anchor][row_block][:, None, None]
        block_allow = visit_rows & doc_match
        context_allow = block_allow[:, :, key_block].reshape(TOK_DEV, (HOPS + 1) * CTX_DEV)
        allowed = jnp.concatenate([context_allow, causal], axis=1)

        def one_head(kv_head):
            query_part = query_heads[anchor][:, kv_head].astype(jnp.float32)
            key_part = all_keys[:, kv_head].astype(jnp.float32)
            value_part = all_values[:, kv_head].astype(jnp.float32)
            scores = jnp.einsum('tjd,sd->tjs', query_part, key_part) * softmax_scale
            scores = jnp.where(allowed[:, None, :], scores, -jnp.inf)
            highest = jnp.max(scores, axis=-1, keepdims=True)
            weights = jnp.exp(scores - highest)
            weight_sum = jnp.sum(weights, axis=-1)
            rounded = lax.optimization_barrier(weights.astype(jnp.bfloat16)).astype(jnp.float32)
            summed = jnp.einsum('tjs,sd->tjd', rounded, value_part)
            return summed / weight_sum[:, :, None]

        heads_out = lax.map(one_head, jnp.arange(KVH))
        return jnp.transpose(heads_out, (1, 0, 2, 3)).reshape(TOK_DEV, HQ * HD).astype(jnp.bfloat16)

    attended = lax.map(one_shard, jnp.arange(N_BLK)).reshape(TOKENS, HQ * HD)
    return jnp.dot(attended, out_weight, preferred_element_type=jnp.float32).astype(jnp.bfloat16)
```

```python
import functools

import jax
import jax.numpy as jnp
from jax import lax
from jax.experimental import pallas as pl
from jax.experimental.pallas import tpu as pltpu
from jax.sharding import Mesh
from jax.sharding import PartitionSpec as P

HQ = 64
KVH = 8
HD = 128
BLOCK = 128
GROUP = HQ // KVH
LOG2E = 1.4426950408889634
SCALE = LOG2E * HD ** (-0.5)
AXES = ("z", "xh", "c", "y", "xl")


def shift(value, axis, by):
    n = lax.axis_size(axis)
    return lax.ppermute(value, axis, [(i, (i + by) % n) for i in range(n)])


def swap(value, axis, mask):
    n = lax.axis_size(axis)
    return lax.ppermute(value, axis, [(i, i ^ mask) for i in range(n)])


def attention_body(
    where, qd, bd, vis, q, ko, vo, k2, v2, ku, vu, ks, vs, rk, rv, out, kc, vc, m_s, l_s, o_s
):
    pos = where[0]
    core = where[1]
    s_u = 1 + 2 * core
    s_s = 3 - 2 * core
    slots = ((ko, vo, 0), (k2, v2, 2), (ku, vu, s_u), (ks, vs, s_s))
    chunks = GROUP // 2

    def step(qb, keys, values, mask, first):
        for hc in range(chunks):
            rows = pl.ds(qb * BLOCK, BLOCK)
            qs = jnp.concatenate(
                [q[rows, (2 * hc + h) * HD : (2 * hc + h + 1) * HD] for h in range(2)], axis=0
            )
            s = lax.dot_general(
                keys, qs, (((1,), (1,)), ((), ())), preferred_element_type=jnp.float32
            )
            s = jnp.where(mask, s * SCALE, -jnp.inf)
            top = jnp.max(s, axis=0, keepdims=True)
            if first:
                m_new = top
            else:
                m_old = m_s[hc]
                m_new = jnp.maximum(m_old, top)
                alpha = jnp.exp2(m_old - m_new)
            p = jnp.exp2(s - m_new)
            total = jnp.sum(p, axis=0, keepdims=True)
            o = lax.dot_general(
                values,
                p.astype(jnp.bfloat16),
                (((0,), (0,)), ((), ())),
                preferred_element_type=jnp.float32,
            )
            m_s[hc] = m_new
            if first:
                l_s[hc] = total
                o_s[hc] = o
            else:
                l_s[hc] = l_s[hc] * alpha + total
                o_s[hc] = o_s[hc] * alpha + o

    for qb in range(2):
        qrow = 2 * pos + qb
        doc = qd[qrow]
        count = jnp.int32(0)
        if qb == 1:
            kc[0:BLOCK, :] = rk[0:BLOCK, :]
            vc[0:BLOCK, :] = rv[0:BLOCK, :]
            count = jnp.int32(1)
        for kref, vref, s in slots:
            holder = (pos + s) % 16

            def pick(j, n, kref=kref, vref=vref, s=s, holder=holder):
                ok = (vis[qrow * 32 + s * 8 + j] == 1) & (bd[holder * 8 + j] == doc)

                @pl.when(ok)
                def _():
                    kc[pl.ds(n * BLOCK, BLOCK), :] = kref[pl.ds(j * BLOCK, BLOCK), :]
                    vc[pl.ds(n * BLOCK, BLOCK), :] = vref[pl.ds(j * BLOCK, BLOCK), :]

                return n + ok.astype(jnp.int32)

            count = lax.fori_loop(0, 8, pick, count)
        kc[pl.ds(count * BLOCK, BLOCK), :] = jnp.zeros((BLOCK, HD), jnp.bfloat16)
        vc[pl.ds(count * BLOCK, BLOCK), :] = jnp.zeros((BLOCK, HD), jnp.bfloat16)
        key_at = lax.broadcasted_iota(jnp.int32, (BLOCK, 2 * BLOCK), 0)
        row_at = lax.broadcasted_iota(jnp.int32, (BLOCK, 2 * BLOCK), 1) % BLOCK
        own = slice(qb * BLOCK, (qb + 1) * BLOCK)
        step(qb, rk[own, :], rv[own, :], key_at <= row_at, True)

        def pair(i, carry, qb=qb, count=count):
            at = pl.ds(i * 2 * BLOCK, 2 * BLOCK)
            left = (count - 2 * i) * BLOCK
            mask = lax.broadcasted_iota(jnp.int32, (2 * BLOCK, 2 * BLOCK), 0) < left
            step(qb, kc[at, :], vc[at, :], mask, False)
            return carry

        lax.fori_loop(0, (count + 1) // 2, pair, 0)
        for hc in range(chunks):
            o = o_s[hc] / l_s[hc]
            for h in range(2):
                head = 2 * hc + h
                out[own, head * HD : (head + 1) * HD] = o[:, h * BLOCK : (h + 1) * BLOCK].T.astype(
                    jnp.bfloat16
                )


def attention(where, qd, bd, vis, q, kv):
    smem = pl.BlockSpec(memory_space=pltpu.SMEM)
    vmem = pl.BlockSpec(memory_space=pltpu.VMEM)
    chunks = GROUP // 2
    return pl.pallas_call(
        attention_body,
        out_shape=jax.ShapeDtypeStruct(q.shape, jnp.bfloat16),
        in_specs=[smem] * 4 + [vmem] * (1 + len(kv)),
        out_specs=vmem,
        scratch_shapes=[
            pltpu.VMEM((36 * BLOCK, HD), jnp.bfloat16),
            pltpu.VMEM((36 * BLOCK, HD), jnp.bfloat16),
            pltpu.VMEM((chunks, 1, 2 * BLOCK), jnp.float32),
            pltpu.VMEM((chunks, 1, 2 * BLOCK), jnp.float32),
            pltpu.VMEM((chunks, HD, 2 * BLOCK), jnp.float32),
        ],
        name="attend",
    )(where, qd, bd, vis, q, *kv)


def project_body(where, *refs):
    a = refs[:4]
    w = refs[4:20]
    out = refs[20]
    wv, sems = refs[21], refs[22]
    copies = [pltpu.make_async_copy(w[i], wv.at[i], sems.at[i]) for i in range(16)]
    for copy in copies:
        copy.start()
    for ahead in range(4):
        to = (where[0] + ahead - where[1] + 4) % 4
        for other in range(2):
            at = (ahead * 2 + other) * 2
            copies[at].wait()
            copies[at + 1].wait()
            for tok in range(2):
                acc = jnp.dot(
                    a[2 * tok][...], wv[at], preferred_element_type=jnp.float32
                ) + jnp.dot(a[2 * tok + 1][...], wv[at + 1], preferred_element_type=jnp.float32)
                out[to, tok, :, other * 256 : (other + 1) * 256] = acc.astype(jnp.bfloat16)


def project(where, a, w):
    smem = pl.BlockSpec(memory_space=pltpu.SMEM)
    vmem = pl.BlockSpec(memory_space=pltpu.VMEM)
    hbm = pl.BlockSpec(memory_space=pl.ANY)
    return pl.pallas_call(
        project_body,
        out_shape=jax.ShapeDtypeStruct((4, 2, 256, 512), jnp.bfloat16),
        in_specs=[smem] + [vmem] * 4 + [hbm] * 16,
        out_specs=vmem,
        scratch_shapes=[
            pltpu.VMEM((16, 1024, 256), jnp.bfloat16),
            pltpu.SemaphoreType.DMA((16,)),
        ],
        name="project",
    )(where, *a, *w)


def add_body(where, p0, p1, p2, p3, out):
    for r in range(2):
        piece = (where[0] + where[1] + r) % 2
        total = (
            p0[piece].astype(jnp.float32)
            + p1[piece].astype(jnp.float32)
            + p2[piece].astype(jnp.float32)
            + p3[piece].astype(jnp.float32)
        )
        out[r] = total.astype(jnp.bfloat16)


def place_body(where, r0, r1, out):
    xh, core = where[0], where[1]
    for r, ref in enumerate((r0, r1)):
        half = (xh + r) % 2
        for other in range(2):
            block = (core + other) % 2
            at = pl.multiple_of(block * 512 + half * 256, 256)
            out[:, pl.ds(at, 256)] = ref[:, other * 256 : (other + 1) * 256]


def small_call(body, name, shape, where, *args):
    smem = pl.BlockSpec(memory_space=pltpu.SMEM)
    vmem = pl.BlockSpec(memory_space=pltpu.VMEM)
    return pl.pallas_call(
        body,
        out_shape=jax.ShapeDtypeStruct(shape, jnp.bfloat16),
        in_specs=[smem] + [vmem] * len(args),
        out_specs=vmem,
        name=name,
    )(where, *args)


def shards(q, ck, cv, rk, rv, w, qd, bd, vis):
    z, xh, c = lax.axis_index("z"), lax.axis_index("xh"), lax.axis_index("c")
    y, xl = lax.axis_index("y"), lax.axis_index("xl")
    pos = (z * 2 + xh) * 2 + c

    k2, v2 = (
        lax.ppermute(t, ("z", "xh"), [(i, (i - 1) % 8) for i in range(8)]) for t in (ck, cv)
    )
    pairs = [(2 * i + 1, 2 * i) for i in range(8)] + [
        (2 * ((i + 2) % 8), 2 * i + 1) for i in range(8)
    ]
    ku, vu = (lax.ppermute(t, ("z", "xh", "c"), pairs) for t in (ck, cv))
    ks, vs = (swap(t, "c", 1) for t in (k2, v2))

    kept = lax.dynamic_slice_in_dim(w, xl * 256, 256, axis=1)
    given = lax.dynamic_slice_in_dim(w, (1 - xl) * 256, 256, axis=1)
    taken = swap(given, "xl", 1)
    w_rel = {}
    for r, part in enumerate((kept, taken)):
        for ahead in range(4):
            mine = part if ahead == 0 else shift(part, "z", -ahead)
            w_rel[ahead, 0, r] = mine
            w_rel[ahead, 1, r] = swap(mine, "c", 1)
    weights = [w_rel[a, o, r] for a in range(4) for o in range(2) for r in range(2)]

    ints = jnp.stack([pos, c]).astype(jnp.int32)
    att = attention(
        ints, qd, bd, vis.reshape(-1), q, (ck, cv, k2, v2, ku, vu, ks, vs, rk, rv)
    )
    x = ("xh", "xl")
    a = [att, swap(att, x, 1), swap(att, x, 2), swap(att, x, 3)]
    part = project(jnp.stack([z, y]).astype(jnp.int32), a, weights)
    pieces = [part[0]] + [shift(part[d], "y", d) for d in range(1, 4)]
    sums = small_call(
        add_body, "add", (2, 256, 512), jnp.stack([xh, xl]).astype(jnp.int32), *pieces
    )
    last = [
        lax.ppermute(
            sums[r], x, [(2 * s + l, 2 * (l ^ r) + s) for s in range(2) for l in range(2)]
        )
        for r in range(2)
    ]
    return small_call(
        place_body, "place", (256, 1024), jnp.stack([xh, c]).astype(jnp.int32), *last
    )


def solution(mesh):
    fine = Mesh(mesh.devices.reshape(4, 2, 2, 4, 2), AXES)
    blk, head = ("z", "xh", "c"), ("y", "xl")
    in_specs = (
        P(blk, head),
        P(blk, head),
        P(blk, head),
        P(blk, head),
        P(blk, head),
        P(head, blk),
        P(),
        P(),
        P(),
    )
    return jax.shard_map(
        shards, mesh=fine, in_specs=in_specs, out_specs=P(blk, head), check_vma=False
    )
```

```python
import jax
import jax.numpy as jnp
from jax import lax
from jax.experimental import pallas as pl
from jax.experimental.pallas import tpu as pltpu
from jax.sharding import Mesh
from jax.sharding import PartitionSpec as P


HQ = 64
KVH = 8
HD = 128
BLOCK = 128
GROUP = HQ // KVH
LOG2E = 1.4426950408889634
SCALE = LOG2E * HD ** (-0.5)
AXES = ("z", "xh", "c", "y", "xl")


def shift(value, axis, by):
    n = lax.axis_size(axis)
    return lax.ppermute(value, axis, [(i, (i + by) % n) for i in range(n)])


def swap(value, axis, mask):
    n = lax.axis_size(axis)
    return lax.ppermute(value, axis, [(i, i ^ mask) for i in range(n)])


CHUNKS = 4
PER = GROUP // CHUNKS
WIDE = PER * BLOCK
CTX = 1024


def attend_pair(one, two, values, qt, m, l, o, first, mask):
    keys = jnp.concatenate([one, two], axis=0)
    values = jnp.concatenate([v.T for v in values], axis=1)
    span = range(CHUNKS)
    s = [jnp.dot(keys, qt[i], preferred_element_type=jnp.float32) for i in span]
    if mask is not None:
        s = [jnp.where(mask, t, -jnp.inf) for t in s]
    m_new = [jnp.max(t, axis=0, keepdims=True) * SCALE for t in s]
    if not first:
        m_old = [m[i] for i in span]
        m_new = [jnp.maximum(m_old[i], m_new[i]) for i in span]
        alpha = [jnp.exp2(m_old[i] - m_new[i]) for i in span]
    p = [jnp.exp2(s[i] * SCALE - m_new[i]) for i in span]
    total = [jnp.sum(t, axis=0, keepdims=True) for t in p]
    part = [jnp.dot(values, t.astype(jnp.bfloat16), preferred_element_type=jnp.float32) for t in p]
    for i in span:
        m[i] = m_new[i]
        l[i] = total[i] if first else l[i] * alpha[i] + total[i]
        o[i] = part[i] if first else o[i] * alpha[i] + part[i]


def block_of(ref, block):
    return ref[pl.ds(pl.multiple_of(block * BLOCK, BLOCK), BLOCK), :]


def pick_blocks(where, qd, bd, vis, picks, qb, count, strides):
    qrow = 2 * where[0] + qb
    doc = qd[qrow]
    for slot, s in enumerate(strides):
        first = ((where[0] + s) % 16) * 8
        for j in range(8):
            ok = (vis[s * 8 + j, qrow] == 1) & (bd[first + j] == doc)
            picks[qb, count] = jnp.int32(slot * 8 + j)
            count = count + ok.astype(jnp.int32)
    return count


def early_body(where, qd, bd, vis, q, ck, cv, rk, rv, qt, m, l, o, kall, vall, picks):
    kall[0:CTX, :] = ck[...]
    kall[CTX:, :] = rk[...]
    vall[0:CTX, :] = cv[...]
    vall[CTX:, :] = rv[...]
    resp = CTX // BLOCK
    for qb in range(2):
        for hc in range(CHUNKS):
            for h in range(PER):
                head = PER * hc + h
                qt[qb, hc, :, h * BLOCK : (h + 1) * BLOCK] = q[
                    qb * BLOCK : (qb + 1) * BLOCK, head * HD : (head + 1) * HD
                ].T
    for qb in range(2):
        count = jnp.int32(qb)
        picks[qb, 0] = jnp.int32(resp)
        count = pick_blocks(where, qd, bd, vis, picks, qb, count, (0,))
        odd = count % 2
        last = jnp.where(odd == 1, picks[qb, jnp.maximum(count - 1, 0)], resp)
        key_at = lax.broadcasted_iota(jnp.int32, (2 * BLOCK, WIDE), 0)
        row_at = lax.broadcasted_iota(jnp.int32, (2 * BLOCK, WIDE), 1) % BLOCK
        row_at = jnp.where(key_at < BLOCK, row_at, odd * 4 * BLOCK - 1)
        state = (qt.at[qb], m.at[qb], l.at[qb], o.at[qb])

        def pair(one, two, first, mask, state=state):
            values = (block_of(vall, one), block_of(vall, two))
            attend_pair(block_of(kall, one), block_of(kall, two), values, *state, first, mask)

        pair(resp + qb, last, True, key_at <= row_at)

        def body(i, carry, qb=qb, pair=pair):
            pair(picks[qb, 2 * i], picks[qb, 2 * i + 1], False, None)
            return carry

        lax.fori_loop(0, count // 2, body, 0)


def attend_body(where, qd, bd, vis, qt, m0, l0, o0, *refs):
    out, kall, vall, m, l, o, picks = refs[6:]
    for i in range(3):
        kall[i * CTX : (i + 1) * CTX, :] = refs[2 * i][...]
        vall[i * CTX : (i + 1) * CTX, :] = refs[2 * i + 1][...]
    m[...] = m0[...]
    l[...] = l0[...]
    o[...] = o0[...]
    core = where[1]
    for qb in range(2):
        strides = (2, 1 + 2 * core, 3 - 2 * core)
        count = pick_blocks(where, qd, bd, vis, picks, qb, jnp.int32(0), strides)
        state = (qt.at[qb], m.at[qb], l.at[qb], o.at[qb])

        def pair(one, two, mask, state=state):
            values = (block_of(vall, one), block_of(vall, two))
            attend_pair(block_of(kall, one), block_of(kall, two), values, *state, False, mask)

        def body(i, carry, qb=qb, pair=pair):
            pair(picks[qb, 2 * i], picks[qb, 2 * i + 1], None)
            return carry

        lax.fori_loop(0, count // 2, body, 0)

        @pl.when(count % 2 == 1)
        def _(qb=qb, pair=pair, count=count):
            last = picks[qb, count - 1]
            pair(last, last, lax.broadcasted_iota(jnp.int32, (2 * BLOCK, WIDE), 0) < BLOCK)

        for hc in range(CHUNKS):
            done = o[qb, hc] * (1.0 / l[qb, hc])
            for h in range(PER):
                head = PER * hc + h
                out[qb * BLOCK : (qb + 1) * BLOCK, head * HD : (head + 1) * HD] = done[
                    :, h * BLOCK : (h + 1) * BLOCK
                ].T.astype(jnp.bfloat16)


SMEM = pl.BlockSpec(memory_space=pltpu.SMEM)
VMEM = pl.BlockSpec(memory_space=pltpu.VMEM)
STATE = (
    jax.ShapeDtypeStruct((2, CHUNKS, 1, WIDE), jnp.float32),
    jax.ShapeDtypeStruct((2, CHUNKS, 1, WIDE), jnp.float32),
    jax.ShapeDtypeStruct((2, CHUNKS, HD, WIDE), jnp.float32),
)


def early(table, q, kv):
    return pl.pallas_call(
        early_body,
        out_shape=(jax.ShapeDtypeStruct((2, CHUNKS, HD, WIDE), jnp.bfloat16), *STATE),
        in_specs=[SMEM] * 4 + [VMEM] * 5,
        out_specs=(VMEM,) * 4,
        scratch_shapes=[
            pltpu.VMEM((CTX + 2 * BLOCK, HD), jnp.bfloat16),
            pltpu.VMEM((CTX + 2 * BLOCK, HD), jnp.bfloat16),
            pltpu.SMEM((2, 16), jnp.int32),
        ],
        compiler_params=pltpu.CompilerParams(vmem_limit_bytes=12 << 20),
        name="early",
    )(*table, q, *kv)


def attend(table, state, kv):
    return pl.pallas_call(
        attend_body,
        out_shape=jax.ShapeDtypeStruct((2 * BLOCK, GROUP * HD), jnp.bfloat16),
        in_specs=[SMEM] * 4 + [VMEM] * 10,
        out_specs=VMEM,
        scratch_shapes=[
            pltpu.VMEM((3 * CTX, HD), jnp.bfloat16),
            pltpu.VMEM((3 * CTX, HD), jnp.bfloat16),
            *[pltpu.VMEM(t.shape, t.dtype) for t in STATE],
            pltpu.SMEM((2, 32), jnp.int32),
        ],
        compiler_params=pltpu.CompilerParams(vmem_limit_bytes=12 << 20),
        name="attend",
    )(*table, *state, *kv)


def project_body(where, *refs):
    a, w, outs = refs[:4], refs[4:13], refs[13:]
    rotation = (where[2] - where[3] + 4) % 4
    for turn in range(4):

        @pl.when(rotation == turn)
        def _(turn=turn):
            for ahead in (0, 3, 1, 2):
                rows = [jnp.concatenate([a[k][...], a[2 + k][...]], axis=0) for k in range(2)]
                if ahead == 2:
                    acc = jnp.dot(rows[0], w[4][...], preferred_element_type=jnp.float32)
                    for part in range(2):
                        acc += jnp.dot(
                            rows[1][:, part * 512 : (part + 1) * 512],
                            w[5 + part][...],
                            preferred_element_type=jnp.float32,
                        )
                else:
                    at = {0: 0, 1: 2, 3: 7}[ahead]
                    acc = jnp.dot(rows[0], w[at][...], preferred_element_type=jnp.float32)
                    acc += jnp.dot(rows[1], w[at + 1][...], preferred_element_type=jnp.float32)
                outs[(ahead + turn) % 4][...] = acc.astype(jnp.bfloat16)


def project(where, a, w):
    return pl.pallas_call(
        project_body,
        out_shape=[jax.ShapeDtypeStruct((512, 256), jnp.bfloat16)] * 4,
        in_specs=[SMEM] + [VMEM] * (4 + len(w)),
        out_specs=[VMEM] * 4,
        compiler_params=pltpu.CompilerParams(vmem_limit_bytes=12 << 20),
    )(where, *[pltpu.with_memory_space_constraint(t, pltpu.VMEM) for t in (*a, *w)])


def add_body(where, p0, p1, p2, p3, *outs):
    for r, out in enumerate(outs):
        half = (where[4] + where[5] + r) % 2
        rows = pl.ds(pl.multiple_of(half * 256, 256), 256)
        total = p0[rows, :].astype(jnp.float32) + p1[rows, :].astype(jnp.float32)
        total += p2[rows, :].astype(jnp.float32) + p3[rows, :].astype(jnp.float32)
        out[...] = total.astype(jnp.bfloat16)


def add(where, pieces):
    return pl.pallas_call(
        add_body,
        out_shape=[jax.ShapeDtypeStruct((256, 256), jnp.bfloat16)] * 2,
        in_specs=[SMEM] + [VMEM] * 4,
        out_specs=[VMEM] * 2,
        compiler_params=pltpu.CompilerParams(vmem_limit_bytes=8 << 20),
    )(where, *pieces)


def place_body(where, *refs):
    out = refs[4]
    for o in range(2):
        for r in range(2):
            at = ((where[1] + o) % 2) * 512 + ((where[4] + r) % 2) * 256
            out[:, pl.ds(pl.multiple_of(at, 256), 256)] = refs[2 * o + r][...]


def place(where, got):
    return pl.pallas_call(
        place_body,
        out_shape=jax.ShapeDtypeStruct((256, 1024), jnp.bfloat16),
        in_specs=[SMEM] + [VMEM] * 4,
        out_specs=VMEM,
        compiler_params=pltpu.CompilerParams(vmem_limit_bytes=8 << 20),
        name="place",
    )(where, *got)


def shards(q, ck, cv, rk, rv, w, qd, bd, vis):
    z, xh, c = lax.axis_index("z"), lax.axis_index("xh"), lax.axis_index("c")
    y, xl = lax.axis_index("y"), lax.axis_index("xl")
    pos = (z * 2 + xh) * 2 + c

    ints = jnp.stack([pos, c, z, y, xh, xl]).astype(jnp.int32)
    table = (ints, qd, bd, vis.transpose(1, 2, 0).reshape(32, 32))

    chips = ("z", "xh")
    ring = [(i, (i - 1) % 8) for i in range(8)]
    pairs = [(2 * i + 1, 2 * i) for i in range(8)]
    pairs += [(2 * ((i + 2) % 8), 2 * i + 1) for i in range(8)]
    k2 = lax.ppermute(ck, chips, ring)
    v2 = lax.ppermute(cv, chips, ring)
    ku = lax.ppermute(ck, ("z", "xh", "c"), pairs)
    vu = lax.ppermute(cv, ("z", "xh", "c"), pairs)
    ks = swap(k2, "c", 1)
    vs = swap(v2, "c", 1)

    kept = lax.dynamic_slice_in_dim(w, xl * 256, 256, axis=1)
    given = lax.dynamic_slice_in_dim(w, (1 - xl) * 256, 256, axis=1)
    taken = swap(given, "xl", 1)
    own = []
    for part, tag in ((kept, "kept"), (taken, "taken")):
        up = shift(part, "z", 1)
        dn = shift(part, "z", -1)
        if tag == "kept":
            far = [shift(up, "z", 1)]
        else:
            far = [shift(up[:512], "z", 1), shift(dn[512:], "z", -1)]
        own.append({"0": part, "1": dn, "3": up})
        own[-1].update({f"2{i}": t for i, t in enumerate(far)})
    keys = [(0, "0"), (1, "0"), (0, "1"), (1, "1"), (0, "20"), (1, "20"), (1, "21"), (0, "3"), (1, "3")]
    weights = [[own[r][k] for r, k in keys]]
    weights.append([swap(own[r][k], "c", 1) for r, k in keys])

    state = early(table, q, (ck, cv, rk, rv))
    att = attend(table, state, (k2, v2, ku, vu, ks, vs))
    x = ("xh", "xl")
    a = [att] + [swap(att, x, m) for m in (1, 2, 3)]
    got = []
    for o in range(2):
        parts = project(ints, a, weights[o])
        pieces = [parts[0]]
        pieces += [shift(parts[d], "y", d) for d in range(1, 4)]
        sums = add(ints, pieces)
        for r in range(2):
            to = [(2 * s + l, 2 * (l ^ r) + s) for s in range(2) for l in range(2)]
            got.append(lax.ppermute(sums[r], x, to))
    return place(ints, got)


def solution(mesh):
    fine = Mesh(mesh.devices.reshape(4, 2, 2, 4, 2), AXES)
    blk, head = ("z", "xh", "c"), ("y", "xl")
    in_specs = (
        P(blk, head),
        P(blk, head),
        P(blk, head),
        P(blk, head),
        P(blk, head),
        P(head, blk),
        P(),
        P(),
        P(),
    )

    return jax.shard_map(
        shards, mesh=fine, in_specs=in_specs, out_specs=P(blk, head), check_vma=False
    )
```
